32 devices in a mesh: groups: 2 (over y), det: 4 (over z), blk: 2 (over x), sub: 2 (over core).
Axes of the slice: x: 2, y: 2, z: 4, core: 2. Of those that a mesh axis runs over, the one named last changes fastest.
Arguments:
- tod: float32 [256, 4, 1024], P(('groups', 'det'), None, ('blk', 'sub')), parts along dimension 0, may hold values from -30 to 30
- pixels: int32 [256, 4, 1024], P('groups', 'det', ('blk', 'sub')), parts along dimension 0, may hold values from 0 to 3071
- span_block: int32 [8, 8], P('groups', ('blk', 'sub')), parts along dimension 0, may hold values from 0 to 7
- weight_class: int32 [256], P('groups'), parts along dimension 0, may hold values from 0 to 7
- class_weight: float32 [16], P('groups'), parts along dimension 0, may hold values from 0.25 to 4
Outputs:
- signal_sum: float32 [16, 3072], P(('groups', 'blk'), ('det', 'sub')), parts along dimension 0
- weight_sum: float32 [16, 3072], P(('groups', 'blk'), ('det', 'sub')), parts along dimension 0
- hit_count: float32 [16, 3072], P(('groups', 'blk'), ('det', 'sub')), parts along dimension 0
The draws below stay inside these ranges and needn't reach their ends.
There are 2 independent parts, one for each index of `groups`. The reference program is written for one: setup_inputs(seed, part) draws one part's arguments, and reference() takes and returns one part's arrays. A program takes and returns all parts, laid end to end along the dimension named above; each array names one. Nothing has to cross between parts.
All inputs are finite; a program needn't handle non-finite values.
Results may differ from the reference program's by a relative error of at most 0.005.
Values sent between devices are 32-bit elements; how exact they have to be, the bound alone decides.
A program may use at most 64 MiB of HBM per device.

```python
import math
import jax
import jax.numpy as jnp
from jax import lax

BLOCK_PIX = 3072
SPAN = 128
NCLASS = 8
NDET = 128
NSEG = 4
SEG = 1024
NCHUNK = 8
NBLOCKS = 8


def shared_integers(key):
    key_base = jax.random.fold_in(key, 29)
    key_perm, key_first, key_second, key_class, key_one, key_two = jax.random.split(key_base, 6)
    block_order = jax.random.permutation(key_perm, NBLOCKS).astype(jnp.int32)
    first_pick = jax.random.randint(key_first, (NSEG, NCHUNK), 0, NBLOCKS, dtype=jnp.int32)
    second_pick = jax.random.randint(key_second, (NSEG, NCHUNK), 0, NBLOCKS, dtype=jnp.int32)
    span_block = block_order[jnp.minimum(first_pick, second_pick)].astype(jnp.int32)
    weight_class = jax.random.randint(key_class, (NDET,), 0, NCLASS, dtype=jnp.int32)
    pick_one = jax.random.randint(key_one, (NDET, NSEG, SEG), 0, BLOCK_PIX, dtype=jnp.int32)
    pick_two = jax.random.randint(key_two, (NDET, NSEG, SEG), 0, BLOCK_PIX, dtype=jnp.int32)
    ranked = jnp.minimum(pick_one, pick_two)
    blocks = jnp.repeat(span_block, SPAN, axis=1)
    shift_block = blocks[None] * 977 * BLOCK_PIX // 3072
    shift_class = weight_class[:, None, None] * 131 * BLOCK_PIX // 3072
    pixels = ((ranked + shift_block + shift_class) % BLOCK_PIX).astype(jnp.int32)
    return (span_block, weight_class, pixels)


def draw_pixels(key, part):
    return shared_integers(key)[2]


def draw_span_block(key, part):
    return shared_integers(key)[0]


def draw_weight_class(key, part):
    return shared_integers(key)[1]


def draw_tod(key, part):
    base = jax.random.fold_in(key, 17)
    key_gain, key_common, key_noise = jax.random.split(base, 3)
    gains = jax.random.uniform(key_gain, (NDET, 1, 1), jnp.float32, 0.5, 1.5)
    common = 3.0 * jax.random.normal(key_common, (1, NSEG, SEG), jnp.float32)
    noise = jax.random.normal(key_noise, (NDET, NSEG, SEG), jnp.float32)
    return jnp.clip(gains * common + noise, -30.0, 30.0)


def setup_inputs(seed: int = 0, part: int = 0) -> dict:
    key_list = jax.random.split(jax.random.key(seed), 6)
    part_splits = jax.random.split(jax.random.fold_in(key_list[5], part), 6)
    tod = draw_tod(jax.random.fold_in(jax.random.fold_in(key_list[5], part), 71), part)
    pixels = draw_pixels(jax.random.fold_in(jax.random.fold_in(key_list[5], part), 71), part)
    span_block = draw_span_block(jax.random.fold_in(jax.random.fold_in(key_list[5], part), 71), part)
    weight_class = draw_weight_class(jax.random.fold_in(jax.random.fold_in(key_list[5], part), 71), part)
    class_weight = jnp.clip(jnp.exp(jax.random.uniform(part_splits[4], (NCLASS,), jnp.float32, math.log(0.25), math.log(4.0))), 0.25, 4.0)
    return {"tod": tod, "pixels": pixels, "span_block": span_block, "weight_class": weight_class, "class_weight": class_weight}


def reference(tod, pixels, span_block, weight_class, class_weight):
    weight = class_weight[weight_class]
    total = jnp.sum(weight)
    common = jnp.sum(weight[:, None, None] * tod, axis=0) / total
    value = (weight[:, None, None] * (tod - common[None])).astype(jnp.bfloat16)
    value = value.astype(jnp.float32)
    weight_low = lax.optimization_barrier(weight.astype(jnp.bfloat16)).astype(jnp.float32)
    blocks = jnp.repeat(span_block, SPAN, axis=1)
    pixel = (blocks[None] * BLOCK_PIX + pixels).astype(jnp.int32).reshape(-1)
    count = NBLOCKS * BLOCK_PIX
    signal_sum = jax.ops.segment_sum(value.reshape(-1), pixel, num_segments=count)
    weight_full = jnp.broadcast_to(weight_low[:, None, None], tod.shape).reshape(-1)
    weight_sum = jax.ops.segment_sum(weight_full, pixel, num_segments=count)
    hit_count = jax.ops.segment_sum(jnp.ones(pixel.shape, jnp.float32), pixel, num_segments=count)
    return (signal_sum.reshape(NBLOCKS, BLOCK_PIX), weight_sum.reshape(NBLOCKS, BLOCK_PIX), hit_count.reshape(NBLOCKS, BLOCK_PIX))
```

```python
import functools

import jax
import jax.numpy as jnp
from jax import lax
from jax.experimental import pallas as pl
from jax.experimental.pallas import tpu as pltpu
from jax.sharding import PartitionSpec as P

BLOCK_PIX = 3072
SPAN = 128
BLK_OWN = 4
TILE = 8
PACK = 16
MESH = pl.DeviceIdType.MESH


def kernel(
    sizes,
    tod_hbm,
    pix_hbm,
    class_hbm,
    class_weight_hbm,
    span_block_hbm,
    out_ref,
    class_ref,
    class_weight_ref,
    span_block_ref,
    tod_in,
    pix_in,
    stage,
    tod_all,
    high_ref,
    low_ref,
    fine_high_ref,
    fine_low_ref,
    weight_rows,
    value_ref,
    early_out,
    early_in,
    late_out,
    late_in,
    load_sem,
    tod_send,
    tod_recv,
    early_send,
    early_recv,
    late_send,
    late_recv,
    passed,
    above,
):
    ndet, nblk, nsub, spans, lanes, rows = sizes
    peers = ndet * nsub
    total_peers = peers * nblk
    mine = tod_hbm.shape[0]
    detectors = ndet * mine
    classes = class_weight_hbm.shape[0]
    det = lax.axis_index("det")
    blk = lax.axis_index("blk")
    sub = lax.axis_index("sub")
    plane_steps = [(db, ds) for db in range(nblk) for ds in range(nsub)]
    plane = [step for step in plane_steps if step != (0, 0)]

    def beside(step, at=None):
        place = {"blk": lax.rem(blk + step[0], nblk), "sub": lax.rem(sub + step[1], nsub)}
        if at is not None:
            place["det"] = at
        return place

    def loads_of(names):
        copies = [pltpu.make_async_copy(a, b, load_sem.at[n]) for n, a, b in names]
        for copy in copies:
            copy.start()
        return copies

    loads = loads_of([(0, tod_hbm, tod_in)])
    barrier = pltpu.get_barrier_semaphore()

    def signal(sem, to):
        pl.semaphore_signal(sem, inc=1, device_id=to, device_id_type=MESH)

    for k in range(ndet - 1, 0, -1):
        pl.when(det + k < ndet)(lambda k=k: signal(barrier, {"det": det + k}))
    pl.when(det > 0)(lambda: signal(barrier, {"det": det - 1}))
    for step in plane:
        signal(barrier, beside(step))
    loads += loads_of(
        [
            (1, pix_hbm, pix_in),
            (2, class_hbm, class_ref),
            (3, class_weight_hbm, class_weight_ref),
            (4, span_block_hbm, span_block_ref),
        ]
    )

    part = mine * spans
    loads[0].wait()
    for seg in range(ndet):
        for span in range(spans):
            stage[seg, pl.ds(span, mine, spans), :] = tod_in[:, seg, span * SPAN : (span + 1) * SPAN]

    def pass_tod(seg):
        pltpu.make_async_remote_copy(
            src_ref=stage.at[seg],
            dst_ref=tod_all.at[det],
            send_sem=tod_send,
            recv_sem=tod_recv,
            device_id={"det": seg},
            device_id_type=MESH,
        ).start()

    def reach(k):
        @pl.when(det + k < ndet)
        def _():
            if k > 1:
                pl.semaphore_wait(above.at[k], 1)
            pass_tod(det + k)
            if k + 1 < ndet:
                pl.when(det > 0)(lambda: signal(above.at[k + 1], {"det": det - 1}))

    pl.semaphore_wait(barrier, len(plane) + det + jnp.where(det + 1 < ndet, 1, 0))
    for k in range(ndet - 1, 0, -1):
        pl.when(det >= k)(lambda k=k: pass_tod(det - k))
    reach(1)
    tod_all[det] = stage[det]
    loads[2].wait()
    loads[3].wait()
    picked = jnp.zeros((1, detectors), jnp.float32)
    for c in range(classes):
        picked = jnp.where(class_ref[...] == c, class_weight_ref[c], picked)
    total = jnp.sum(picked, axis=1, keepdims=True)
    turned = jnp.transpose(jnp.broadcast_to(picked, (SPAN, detectors)))
    for span in range(spans):
        weight_rows[pl.ds(span, detectors, spans), :] = turned

    loads[1].wait()
    pixel = pix_in[...].astype(jnp.float32)
    high = jnp.floor((pixel + 0.5) * (1.0 / lanes))
    high_ref[...] = high
    low = pixel - high * lanes
    low_ref[...] = low
    upper = jnp.where(low >= lanes // 2, 1.0, 0.0)
    fine_high_ref[...] = 2.0 * high + upper
    fine_low_ref[...] = low - upper * (lanes // 2)

    height = peers * TILE
    fine = lanes // 2
    fine_rows = 2 * rows
    field = SPAN // spans
    low_tiles = -(-lanes // PACK)

    def iota(tile):
        return lax.broadcasted_iota(jnp.int32, (PACK, SPAN), 0) + tile * PACK

    def to_low(x):
        return x.astype(jnp.float32).astype(jnp.bfloat16)

    low_ids = [to_low(iota(t)) for t in range(SPAN // PACK)]
    early_ids = []
    late_ids = []
    for t in range(height // PACK):
        row = iota(t)
        peer = row // TILE
        within = row % TILE
        kind = jnp.where(within < rows, within, within - rows)
        early_ids.append(to_low(jnp.where(within < 2 * rows, peer * rows + kind, -1)))
    for t in range(height // PACK):
        row = iota(t)
        within = row % TILE
        late_ids.append(to_low(jnp.where(within < fine_rows, row // TILE * fine_rows + within, -1)))
    is_weight = to_low(jnp.where(iota(0) % TILE < rows, 1, 0)) > 0.5
    one = jnp.ones((PACK, SPAN), jnp.bfloat16)
    zero = jnp.zeros((PACK, SPAN), jnp.bfloat16)

    def spread(ref, row):
        return jnp.broadcast_to(ref[pl.ds(row, 1), :], (PACK, SPAN)).astype(jnp.bfloat16)

    def hot(ids, where, filled):
        return jnp.concatenate([jnp.where(i == where, filled, zero) for i in ids], axis=0)

    chunk = min(64, detectors)

    def contract(left, right):
        return lax.dot_general(
            jnp.concatenate(left, axis=1),
            jnp.concatenate(right, axis=1),
            (((1,), (1,)), ((), ())),
            preferred_element_type=jnp.float32,
        )

    def early_step(i, sums):
        base = pl.multiple_of(i * chunk * spans, TILE)
        new = []
        for span in range(spans):
            left, right = [], []
            for d in range(chunk):
                r = base + d * spans + span
                right.append(hot(low_ids, spread(low_ref, r), one))
                filled = jnp.where(is_weight, spread(weight_rows, r), one)
                left.append(hot(early_ids, spread(high_ref, r), filled))
            new.append(sums[span] + contract(left, right))
        return tuple(new)

    start = tuple(jnp.zeros((height, SPAN), jnp.float32) for _ in range(spans))
    steps = detectors // chunk
    sums = lax.fori_loop(0, steps // 2, early_step, start)
    reach(2)
    sums = lax.fori_loop(steps // 2, steps, early_step, sums)
    for k in range(3, ndet):
        reach(k)
    for step in plane:
        signal(passed, beside(step))
    loads[4].wait()
    label_row = lax.broadcasted_iota(jnp.int32, (TILE, SPAN), 0) == 2 * rows
    for span in range(spans):
        label = span_block_ref[span, det].astype(jnp.float32)
        for p in range(peers):
            tile = sums[span][p * TILE : (p + 1) * TILE]
            early_out[p, span] = jnp.where(label_row, label, tile)

    me = (det * nblk + blk) * nsub + sub

    def ranked(j):
        high = ndet - 1 - j
        low = jnp.where(j >= det, j + 1, j)
        return jnp.where(2 * det < ndet, jnp.where(high <= det, high - 1, high), low)

    def send(source, landing, send_sem, recv_sem, count):
        targets = [beside(step, ranked(j)) for j in range(ndet - 1) for step in plane_steps]
        targets += [beside(step, det) for step in plane]
        for to in targets:
            pltpu.make_async_remote_copy(
                src_ref=source.at[to["det"] * nsub + to["sub"], *count],
                dst_ref=landing.at[me, *count],
                send_sem=send_sem,
                recv_sem=recv_sem,
                device_id=to,
                device_id_type=MESH,
            ).start()

    own_place = det * nsub + sub
    remote = total_peers - 1

    tod_gone = stage.at[pl.ds(0, ndet - 1)]
    pltpu.make_async_copy(tod_gone, tod_all.at[pl.ds(0, ndet - 1)], tod_recv).wait()
    pl.semaphore_wait(passed, len(plane))
    send(early_out, early_in, early_send, early_recv, ())

    period = TILE
    folded = jnp.zeros((period, SPAN), jnp.float32)
    for q in range(ndet):
        weighted = tod_all[q] * weight_rows[q * part : (q + 1) * part]
        for k in range(part // period):
            folded = folded + weighted[k * period : (k + 1) * period]
    shift = spans
    while shift < period:
        folded = folded + pltpu.roll(folded, shift, 0)
        shift *= 2
    common = folded / total
    for q in range(ndet):
        piece = slice(q * part, (q + 1) * part)
        repeated = jnp.concatenate([common] * (part // period), axis=0)
        value_ref[piece] = weight_rows[piece] * (tod_all[q] - repeated)

    def late_step(i, sums):
        base = pl.multiple_of(i * chunk * spans, TILE)
        new = []
        for span in range(spans):
            left, right = [], []
            for d in range(chunk):
                r = base + d * spans + span
                right.append(hot(low_ids[: field // PACK], spread(fine_low_ref, r), one))
                left.append(hot(late_ids, spread(fine_high_ref, r), spread(value_ref, r)))
            new.append(sums[span] + contract(left, right))
        return tuple(new)

    start = tuple(jnp.zeros((height, field), jnp.float32) for _ in range(spans))
    late = lax.fori_loop(0, detectors // chunk, late_step, start)
    for p in range(peers):
        tiles = [late[span][p * TILE : (p + 1) * TILE] for span in range(spans)]
        late_out[p] = jnp.concatenate(tiles, axis=1)
    used = (pl.ds(0, fine_rows),)
    send(late_out, late_in, late_send, late_recv, used)
    late_in[me] = late_out[own_place]
    early_in[me] = early_out[own_place]
    late_bytes = late_in.at[pl.ds(0, remote), *used]

    pltpu.make_async_copy(early_in.at[pl.ds(0, remote)], early_in.at[pl.ds(0, remote)], early_recv).wait()
    first = (blk * BLK_OWN).astype(jnp.float32)

    def gather_early(n, acc):
        acc = list(acc)
        for span in range(spans):
            tile = early_in[n, span]
            label = jnp.broadcast_to(early_in[n, span, pl.ds(2 * rows, 1), :], (TILE, SPAN))
            for b in range(BLK_OWN):
                acc[b] = acc[b] + jnp.where(label == first + b, tile, 0.0)
        return tuple(acc)

    lane = lax.broadcasted_iota(jnp.int32, (TILE, SPAN), 1)

    def gather_late(n, acc):
        label = jnp.broadcast_to(early_in[n, 0, pl.ds(2 * rows, 1), :], (TILE, SPAN))
        for span in range(1, spans):
            other = jnp.broadcast_to(early_in[n, span, pl.ds(2 * rows, 1), :], (TILE, SPAN))
            label = jnp.where(lane < span * field, label, other)
        tile = late_in[n]
        return tuple(
            acc[b] + jnp.where(label == first + b, tile, 0.0) for b in range(BLK_OWN)
        )

    def over_slots(step):
        acc = tuple(jnp.zeros((TILE, SPAN), jnp.float32) for _ in range(BLK_OWN))
        if total_peers <= 16:
            for n in range(total_peers):
                acc = step(n, acc)
            return acc
        return lax.fori_loop(0, total_peers, step, acc)

    acc = over_slots(gather_early)
    for b in range(BLK_OWN):
        for r in range(rows):
            at = slice(r * lanes, (r + 1) * lanes)
            out_ref[1, b : b + 1, at] = acc[b][r : r + 1, :lanes]
            out_ref[2, b : b + 1, at] = acc[b][rows + r : rows + r + 1, :lanes]

    pltpu.make_async_copy(late_bytes, late_bytes, late_recv).wait()
    acc = over_slots(gather_late)
    for b in range(BLK_OWN):
        whole = acc[b]
        for span in range(1, spans):
            whole = whole + pltpu.roll(acc[b], span * field, 1)
        for r in range(fine_rows):
            skip = r * fine % SPAN // field * field
            skip = skip if skip + fine <= SPAN else 0
            line = whole[r : r + 1, skip : skip + fine]
            out_ref[0, b : b + 1, r * fine : (r + 1) * fine] = line

    pltpu.make_async_copy(tod_gone, tod_all.at[pl.ds(0, ndet - 1)], tod_send).wait()
    pltpu.make_async_copy(early_in.at[pl.ds(0, remote)], early_in.at[pl.ds(0, remote)], early_send).wait()
    pltpu.make_async_copy(late_bytes, late_bytes, late_send).wait()


def on_device(tod, pixels, span_block, weight_class, class_weight):
    ndet, nblk, nsub = (lax.axis_size(a) for a in ("det", "blk", "sub"))
    mine, segments, samples = tod.shape
    detectors = pixels.shape[0]
    spans = samples // SPAN
    peers = ndet * nsub
    slots = peers * nblk
    width = BLOCK_PIX // peers
    lanes = next(n for n in range(SPAN, 0, -1) if width % n == 0)
    rows = width // lanes
    assert segments == ndet and detectors == ndet * mine
    assert TILE % spans == 0 and 2 * rows < TILE and lanes % 2 == 0 and lanes // 2 <= SPAN // spans
    flat = (detectors * spans, SPAN)
    vmem = pl.BlockSpec(memory_space=pltpu.VMEM)
    hbm = pl.BlockSpec(memory_space=pl.ANY)
    f32 = jnp.float32
    dma = pltpu.SemaphoreType.DMA
    out = pl.pallas_call(
        functools.partial(kernel, (ndet, nblk, nsub, spans, lanes, rows)),
        out_shape=pltpu.VMEM((3, BLK_OWN, width), f32),
        in_specs=[hbm] * 5,
        out_specs=vmem,
        scratch_shapes=[
            pltpu.VMEM((1, detectors), jnp.int32),
            pltpu.SMEM(class_weight.shape, f32),
            pltpu.SMEM((spans, segments), jnp.int32),
            pltpu.VMEM(tod.shape, f32),
            pltpu.VMEM(flat, jnp.int32),
            pltpu.VMEM((ndet, mine * spans, SPAN), f32),
            pltpu.VMEM((ndet, mine * spans, SPAN), f32),
            pltpu.VMEM(flat, f32),
            pltpu.VMEM(flat, f32),
            pltpu.VMEM(flat, f32),
            pltpu.VMEM(flat, f32),
            pltpu.VMEM(flat, f32),
            pltpu.VMEM(flat, f32),
            pltpu.VMEM((peers, spans, TILE, SPAN), f32),
            pltpu.VMEM((slots, spans, TILE, SPAN), f32),
            pltpu.VMEM((peers, TILE, SPAN), f32),
            pltpu.VMEM((slots, TILE, SPAN), f32),
            dma((5,)),
            dma,
            dma,
            dma,
            dma,
            dma,
            dma,
            pltpu.SemaphoreType.REGULAR,
            pltpu.SemaphoreType.REGULAR((ndet,)),
        ],
        compiler_params=pltpu.CompilerParams(collective_id=0, has_side_effects=True),
    )(
        tod,
        pixels.reshape(flat),
        weight_class.reshape(1, detectors),
        class_weight,
        span_block.T,
    )
    return (out[0], out[1], out[2])


def solution(mesh):
    placed = (
        P(("groups", "det"), None, ("blk", "sub")),
        P("groups", "det", ("blk", "sub")),
        P("groups", ("blk", "sub")),
        P("groups"),
        P("groups"),
    )
    sliced = P(("groups", "blk"), ("det", "sub"))
    return jax.shard_map(
        on_device,
        mesh=mesh,
        in_specs=placed,
        out_specs=(sliced, sliced, sliced),
        check_vma=False,
    )
```

```python
import functools

import jax
import jax.numpy as jnp
from jax import lax
from jax.experimental import pallas as pl
from jax.experimental.pallas import tpu as pltpu
from jax.sharding import PartitionSpec as P

BLOCK_PIX = 3072
SPAN = 128
BLK_OWN = 4
TILE = 8
PACK = 16
CHUNK = 96
TIMES = 32
MESH = pl.DeviceIdType.MESH


def kernel(
    sizes,
    tod_hbm,
    pix_hbm,
    class_hbm,
    class_weight_hbm,
    span_block_hbm,
    out_ref,
    class_ref,
    class_weight_ref,
    span_block_ref,
    tod_in,
    pix_in,
    stage,
    tod_all,
    high_ref,
    low_ref,
    turned_high,
    turned_low,
    weight_rows,
    value_ref,
    moment_ref,
    shift_ref,
    near_ref,
    early_out,
    early_in,
    late_out,
    late_in,
    load_sem,
    tod_send,
    tod_recv,
    early_send,
    early_recv,
    late_send,
    late_recv,
    passed,
):
    ndet, nblk, nsub, spans, lanes, rows = sizes
    peers = ndet * nsub
    total_peers = peers * nblk
    mine = tod_hbm.shape[0]
    detectors = ndet * mine
    classes = class_weight_hbm.shape[0]
    det = lax.axis_index("det")
    blk = lax.axis_index("blk")
    sub = lax.axis_index("sub")
    others = [
        (db, dd, ds)
        for dd in range(ndet)
        for db in range(nblk)
        for ds in range(nsub)
        if (db, dd, ds) != (0, 0, 0)
    ]

    def target(offset):
        db, dd, ds = offset
        return {
            "det": lax.rem(det + dd, ndet),
            "blk": lax.rem(blk + db, nblk),
            "sub": lax.rem(sub + ds, nsub),
        }

    barrier = pltpu.get_barrier_semaphore()
    plane = [offset for offset in others if offset[1] == 0]
    column = [offset for offset in others if offset[0] == 0 and offset[2] == 0]
    for offset in plane + column:
        pl.semaphore_signal(barrier, inc=1, device_id=target(offset), device_id_type=MESH)

    sources = (tod_hbm, pix_hbm, class_hbm, class_weight_hbm, span_block_hbm)
    landings = (tod_in, pix_in, class_ref, class_weight_ref, span_block_ref)
    loads = [
        pltpu.make_async_copy(source, landing, load_sem.at[n])
        for n, (source, landing) in enumerate(zip(sources, landings))
    ]
    for load in loads:
        load.start()

    part = mine * spans
    height = peers * TILE
    fine = lanes // 2
    fine_rows = 2 * rows
    field = SPAN // spans

    loads[0].wait()
    for seg in range(ndet):
        for span in range(spans):
            stage[seg, pl.ds(span, mine, spans), :] = tod_in[:, seg, span * SPAN : (span + 1) * SPAN]

    pl.semaphore_wait(barrier, len(plane + column))
    for high in range(ndet - 1, 0, -1):
        seg = jnp.where(high > det, high, high - 1)
        seg = jnp.where((det == 0) & (seg < ndet - 1), ndet - 1 - seg, seg)
        pltpu.make_async_remote_copy(
            src_ref=stage.at[seg],
            dst_ref=tod_all.at[det],
            send_sem=tod_send,
            recv_sem=tod_recv.at[det],
            device_id={"det": seg},
            device_id_type=MESH,
        ).start()
    for offset in plane:
        pl.semaphore_signal(passed, inc=1, device_id=target(offset), device_id_type=MESH)
    tod_all[det] = stage[det]

    loads[2].wait()
    loads[3].wait()
    picked = jnp.zeros((1, detectors), jnp.float32)
    for c in range(classes):
        picked = jnp.where(class_ref[...] == c, class_weight_ref[c], picked)
    turned = jnp.transpose(jnp.broadcast_to(picked, (SPAN, detectors)))
    for span in range(spans):
        weight_rows[pl.ds(span, detectors, spans), :] = turned

    def place(pixel):
        high = jnp.floor((pixel + 0.5) * (1.0 / fine))
        return high, pixel - high * fine

    loads[1].wait()
    high_ref[...], low_ref[...] = place(pix_in[...].astype(jnp.float32))
    for span in range(spans):
        across = jnp.transpose(pix_in[pl.ds(span, detectors, spans), :].astype(jnp.float32))
        turned_high[span], turned_low[span] = place(across)

    def to_low(x):
        return x.astype(jnp.float32).astype(jnp.bfloat16)

    def ids_of(width):
        def iota(tile):
            return lax.broadcasted_iota(jnp.int32, (PACK, width), 0) + tile * PACK

        low = [to_low(iota(t)) for t in range(field // PACK)]
        high = []
        for t in range(height // PACK):
            within = iota(t) % TILE
            high.append(to_low(jnp.where(within < fine_rows, iota(t) // TILE * fine_rows + within, -1)))
        one = jnp.ones((PACK, width), jnp.bfloat16)
        return low, high, one, jnp.zeros((PACK, width), jnp.bfloat16)

    def hot(ids, where, filled, zero):
        return jnp.concatenate([jnp.where(i == where, filled, zero) for i in ids], axis=0)

    def contract(left, right):
        return lax.dot_general(left, right, (((1,), (1,)), ((), ())), preferred_element_type=jnp.float32)

    low_ids, high_ids, one, zero = ids_of(detectors)
    blank = jnp.zeros((field, detectors), jnp.bfloat16)
    weight_low = jnp.broadcast_to(picked, (PACK, detectors)).astype(jnp.bfloat16)
    times = min(TIMES, SPAN)

    def early_step(i, sums):
        base = pl.multiple_of(i * times, times)
        for n in range(times):
            left, right = [], []
            for span in range(spans):

                def across(ref):
                    return jnp.broadcast_to(ref[span, pl.ds(base + n, 1), :], (PACK, detectors)).astype(jnp.bfloat16)

                hit = hot(low_ids, across(turned_low), one, zero)
                right.append(jnp.concatenate([hit if s == span else blank for s in range(spans)], axis=0))
                where = across(turned_high)
                left.append(
                    jnp.concatenate(
                        [hot(high_ids, where, weight_low, zero), hot(high_ids, where, one, zero)], axis=0
                    )
                )
            new = contract(jnp.concatenate(left, axis=1), jnp.concatenate(right, axis=1))
            moment_ref[base + n] = new[:height]
            sums = sums + new
        return sums

    sums = lax.fori_loop(0, SPAN // times, early_step, jnp.zeros((2 * height, SPAN), jnp.float32))

    lane = lax.broadcasted_iota(jnp.int32, (TILE, SPAN), 1)
    label_row = lax.broadcasted_iota(jnp.int32, (TILE, SPAN), 0) == fine_rows
    loads[4].wait()
    label = jnp.zeros((TILE, SPAN), jnp.float32)
    for span in range(spans):
        label = jnp.where(lane >= span * field, span_block_ref[span, det].astype(jnp.float32), label)
    for p in range(peers):
        early_out[p, 0] = jnp.where(label_row, label, sums[p * TILE : (p + 1) * TILE])
        early_out[p, 1] = sums[height + p * TILE : height + (p + 1) * TILE]

    slot_of = {offset: n for n, offset in enumerate(others)}

    def send(source, landing, send_sem, recv_sem, count):
        for offset in others:
            to = target(offset)
            pltpu.make_async_remote_copy(
                src_ref=source.at[to["det"] * nsub + to["sub"], *count],
                dst_ref=landing.at[slot_of[offset], *count],
                send_sem=send_sem,
                recv_sem=recv_sem,
                device_id=to,
                device_id_type=MESH,
            ).start()

    own_place = det * nsub + sub
    remote = len(others)

    pl.semaphore_wait(passed, len(plane))
    send(early_out, early_in, early_send, early_recv, ())

    far = jnp.where(det > 0, 0, ndet - 1)
    first_near = jnp.where(det > 0, 1, 0)

    def arrived(q):
        pltpu.make_async_copy(stage.at[0], tod_all.at[q], tod_recv.at[q]).wait()

    def rows_of(q):
        return pl.ds(pl.multiple_of(q * part, TILE), part)

    def fold(total, q):
        weighted = tod_all[q] * weight_rows[rows_of(q), :]
        for k in range(part // TILE):
            total = total + weighted[k * TILE : (k + 1) * TILE]
        return total

    def over_spans(folded):
        shift = spans
        while shift < TILE:
            folded = folded + pltpu.roll(folded, shift, 0)
            shift *= 2
        return folded

    def form(q, level):
        repeated = jnp.concatenate([level] * (part // TILE), axis=0)
        value_ref[rows_of(q), :] = weight_rows[rows_of(q), :] * (tod_all[q] - repeated)

    near = [first_near + k for k in range(ndet - 1)]
    folded = jnp.zeros((TILE, SPAN), jnp.float32)
    for q in near:
        pl.when(q != det)(functools.partial(arrived, q))
        folded = fold(folded, q)
    source = lax.broadcasted_iota(jnp.int32, (1, detectors), 1) // mine
    near_total = jnp.sum(jnp.where(source == far, 0.0, picked), axis=1, keepdims=True)
    total = jnp.sum(picked, axis=1, keepdims=True)
    level = over_spans(folded) / near_total
    for q in near:
        form(q, level)

    row_low, row_high, row_one, row_zero = ids_of(SPAN)

    def spread(ref, row):
        return jnp.broadcast_to(ref[pl.ds(row, 1), :], (PACK, SPAN)).astype(jnp.bfloat16)

    def value_sums(first, count, sums):
        base = pl.multiple_of(first * spans, TILE)
        new = []
        for span in range(spans):
            left, right = [], []
            for d in range(count):
                r = base + d * spans + span
                right.append(hot(row_low, spread(low_ref, r), row_one, row_zero))
                left.append(hot(row_high, spread(high_ref, r), spread(value_ref, r), row_zero))
            both = contract(jnp.concatenate(left, axis=1), jnp.concatenate(right, axis=1))
            new.append(sums[span] + both)
        return tuple(new)

    nearby = (ndet - 1) * mine
    chunk = max(c for c in range(mine, CHUNK + 1, mine) if nearby % c == 0)
    start = tuple(jnp.zeros((height, field), jnp.float32) for _ in range(spans))
    late = lax.fori_loop(
        0,
        nearby // chunk,
        lambda i, sums: value_sums(first_near * mine + i * chunk, chunk, sums),
        start,
    )

    near_ref[...] = jnp.concatenate(late, axis=1)
    arrived(far)
    folded = fold(folded, far)
    form(far, level)
    change = over_spans(folded) / total - level
    by_lane = [jnp.broadcast_to(change[span : span + 1], (field, SPAN)) for span in range(spans)]
    shift_ref[...] = jnp.transpose(jnp.concatenate(by_lane, axis=0))
    late = value_sums(far * mine, mine, start)
    signal = near_ref[...] + jnp.concatenate(late, axis=1)
    moved = [jnp.zeros((height, SPAN), jnp.float32) for _ in range(2)]
    for t in range(SPAN):
        by = jnp.broadcast_to(shift_ref[t : t + 1, :], (height, SPAN))
        moved[t % 2] = moved[t % 2] + by * moment_ref[t]
    signal = signal - (moved[0] + moved[1])
    for p in range(peers):
        late_out[p] = signal[p * TILE : (p + 1) * TILE]
    used = (pl.ds(0, fine_rows),)
    send(late_out, late_in, late_send, late_recv, used)
    late_in[remote] = late_out[own_place]
    early_in[remote] = early_out[own_place]

    def finish(copy_sem, landing):
        pltpu.make_async_copy(landing, landing, copy_sem).wait()

    early_all = early_in.at[pl.ds(0, remote)]
    late_all = late_in.at[pl.ds(0, remote), *used]
    first = (blk * BLK_OWN).astype(jnp.float32)

    def gather(tiles_of):
        def step(n, acc):
            label = jnp.broadcast_to(early_in[n, 0, pl.ds(fine_rows, 1), :], (TILE, SPAN))
            acc = list(acc)
            for b in range(BLK_OWN):
                mine_here = label == first + b
                for k, tile in enumerate(tiles_of(n)):
                    at = k * BLK_OWN + b
                    acc[at] = acc[at] + jnp.where(mine_here, tile, 0.0)
            return tuple(acc)

        kinds = len(tiles_of(0))
        acc = tuple(jnp.zeros((TILE, SPAN), jnp.float32) for _ in range(kinds * BLK_OWN))
        if total_peers <= 16:
            for n in range(total_peers):
                acc = step(n, acc)
            return acc
        return lax.fori_loop(0, total_peers, step, acc)

    def put(kind, tiles):
        for b, tile in enumerate(tiles):
            whole = tile
            for span in range(1, spans):
                whole = whole + pltpu.roll(tile, span * field, 1)
            for r in range(fine_rows):
                skip = r * fine % SPAN // field * field
                skip = skip if skip + fine <= SPAN else 0
                line = whole[r : r + 1, skip : skip + fine]
                out_ref[kind, b : b + 1, r * fine : (r + 1) * fine] = line

    finish(early_recv, early_all)
    acc = gather(lambda n: (early_in[n, 0], early_in[n, 1]))
    put(1, acc[:BLK_OWN])
    put(2, acc[BLK_OWN:])

    finish(late_recv, late_all)
    put(0, gather(lambda n: (late_in[n],)))

    tod_gone = tod_all.at[pl.ds(0, ndet - 1)]
    finish(tod_send, tod_gone)
    finish(early_send, early_all)
    finish(late_send, late_all)


def on_device(tod, pixels, span_block, weight_class, class_weight):
    ndet, nblk, nsub = (lax.axis_size(a) for a in ("det", "blk", "sub"))
    mine, segments, samples = tod.shape
    detectors = pixels.shape[0]
    spans = samples // SPAN
    peers = ndet * nsub
    slots = peers * nblk
    width = BLOCK_PIX // peers
    lanes = next(n for n in range(SPAN, 0, -1) if width % n == 0)
    rows = width // lanes
    assert segments == ndet and detectors == ndet * mine
    assert TILE % spans == 0 and 2 * rows < TILE and lanes % 2 == 0 and lanes // 2 <= SPAN // spans
    flat = (detectors * spans, SPAN)
    vmem = pl.BlockSpec(memory_space=pltpu.VMEM)
    hbm = pl.BlockSpec(memory_space=pl.ANY)
    f32 = jnp.float32
    dma = pltpu.SemaphoreType.DMA
    out = pl.pallas_call(
        functools.partial(kernel, (ndet, nblk, nsub, spans, lanes, rows)),
        out_shape=pltpu.VMEM((3, BLK_OWN, width), f32),
        in_specs=[hbm] * 5,
        out_specs=vmem,
        scratch_shapes=[
            pltpu.VMEM((1, detectors), jnp.int32),
            pltpu.SMEM(class_weight.shape, f32),
            pltpu.SMEM((spans, segments), jnp.int32),
            pltpu.VMEM(tod.shape, f32),
            pltpu.VMEM(flat, jnp.int32),
            pltpu.VMEM((ndet, mine * spans, SPAN), f32),
            pltpu.VMEM((ndet, mine * spans, SPAN), f32),
            pltpu.VMEM(flat, f32),
            pltpu.VMEM(flat, f32),
            pltpu.VMEM((spans, SPAN, detectors), f32),
            pltpu.VMEM((spans, SPAN, detectors), f32),
            pltpu.VMEM(flat, f32),
            pltpu.VMEM(flat, f32),
            pltpu.VMEM((SPAN, peers * TILE, SPAN), f32),
            pltpu.VMEM((SPAN, SPAN), f32),
            pltpu.VMEM((peers * TILE, SPAN), f32),
            pltpu.VMEM((peers, 2, TILE, SPAN), f32),
            pltpu.VMEM((slots, 2, TILE, SPAN), f32),
            pltpu.VMEM((peers, TILE, SPAN), f32),
            pltpu.VMEM((slots, TILE, SPAN), f32),
            dma((5,)),
            dma,
            dma((ndet,)),
            dma,
            dma,
            dma,
            dma,
            pltpu.SemaphoreType.REGULAR,
        ],
        compiler_params=pltpu.CompilerParams(collective_id=0, has_side_effects=True),
    )(
        tod,
        pixels.reshape(flat),
        weight_class.reshape(1, detectors),
        class_weight,
        span_block.T,
    )
    return (out[0], out[1], out[2])


def solution(mesh):
    placed = (
        P(("groups", "det"), None, ("blk", "sub")),
        P("groups", "det", ("blk", "sub")),
        P("groups", ("blk", "sub")),
        P("groups"),
        P("groups"),
    )
    sliced = P(("groups", "blk"), ("det", "sub"))
    return jax.shard_map(
        on_device,
        mesh=mesh,
        in_specs=placed,
        out_specs=(sliced, sliced, sliced),
        check_vma=False,
    )
```

```python
import functools

import jax
import jax.numpy as jnp
from jax import lax
from jax.experimental import pallas as pl
from jax.experimental.pallas import tpu as pltpu
from jax.sharding import PartitionSpec as P

BLOCK_PIX = 3072
SPAN = 128
BLK_OWN = 4
TILE = 8
PACK = 16
EARLY = 64
LATE = 128
MESH = pl.DeviceIdType.MESH


def kernel(
    sizes,
    tod_hbm,
    pix_hbm,
    class_hbm,
    class_weight_hbm,
    span_block_hbm,
    out_ref,
    class_ref,
    class_weight_ref,
    span_block_ref,
    pix_in,
    stage,
    tod_all,
    high_ref,
    low_ref,
    weight_rows,
    value_ref,
    early_flat,
    held,
    early_out,
    early_in,
    late_out,
    late_in,
    load_sem,
    tod_send,
    tod_recv,
    early_send,
    early_recv,
    late_send,
    late_recv,
    passed,
):
    ndet, nblk, nsub, spans, lanes, rows = sizes
    peers = ndet * nsub
    total_peers = peers * nblk
    mine = tod_hbm.shape[0]
    detectors = ndet * mine
    classes = class_weight_hbm.shape[0]
    det = lax.axis_index("det")
    blk = lax.axis_index("blk")
    sub = lax.axis_index("sub")
    others = [
        (db, dd, ds)
        for dd in range(ndet)
        for db in range(nblk)
        for ds in range(nsub)
        if (db, dd, ds) != (0, 0, 0)
    ]

    def target(offset):
        db, dd, ds = offset
        return {
            "det": lax.rem(det + dd, ndet),
            "blk": lax.rem(blk + db, nblk),
            "sub": lax.rem(sub + ds, nsub),
        }

    for seg in range(ndet):
        for span in range(spans):
            pltpu.make_async_copy(
                tod_hbm.at[:, seg, pl.ds(span * SPAN, SPAN)], stage.at[seg, span], load_sem.at[0]
            ).start()

    barrier = pltpu.get_barrier_semaphore()
    plane = [offset for offset in others if offset[1] == 0]
    column = [offset for offset in others if offset[0] == 0 and offset[2] == 0]
    for offset in column + plane:
        pl.semaphore_signal(barrier, inc=1, device_id=target(offset), device_id_type=MESH)

    sources = (pix_hbm, class_hbm, class_weight_hbm, span_block_hbm)
    landings = (pix_in, class_ref, class_weight_ref, span_block_ref)
    loads = [
        pltpu.make_async_copy(source, landing, load_sem.at[n + 1])
        for n, (source, landing) in enumerate(zip(sources, landings))
    ]
    for load in loads:
        load.start()

    height = peers * TILE
    group = 4 * rows
    tall = -(-peers * group // PACK) * PACK
    fine = lanes // 2
    fine_rows = 2 * rows
    field = SPAN // spans

    pltpu.make_async_copy(stage, stage, load_sem.at[0]).wait()
    pl.semaphore_wait(barrier, len(plane + column))
    for span in range(spans):
        for high in range(ndet - 1, 0, -1):
            seg = jnp.where(high > det, high, high - 1)
            seg = jnp.where((det == 0) & (seg < ndet - 1), ndet - 1 - seg, seg)
            pltpu.make_async_remote_copy(
                src_ref=stage.at[seg, span],
                dst_ref=tod_all.at[det, span],
                send_sem=tod_send,
                recv_sem=tod_recv.at[span],
                device_id={"det": seg},
                device_id_type=MESH,
            ).start()
    for offset in plane:
        pl.semaphore_signal(passed, inc=1, device_id=target(offset), device_id_type=MESH)
    tod_all[det] = stage[det]

    loads[1].wait()
    loads[2].wait()
    picked = jnp.zeros((1, detectors), jnp.float32)
    for c in range(classes):
        picked = jnp.where(class_ref[...] == c, class_weight_ref[c], picked)
    weight_rows[...] = jnp.transpose(jnp.broadcast_to(picked, (SPAN, detectors)))

    def place(pixel):
        high = jnp.floor((pixel + 0.5) * (1.0 / fine))
        return high, pixel - high * fine

    loads[0].wait()
    for span in range(spans):
        pixel = pix_in[pl.ds(span, detectors, spans), :].astype(jnp.float32)
        high_ref[span], low_ref[span] = place(pixel)

    def to_low(x):
        return x.astype(jnp.float32).astype(jnp.bfloat16)

    def iota(tile):
        return lax.broadcasted_iota(jnp.int32, (PACK, SPAN), 0) + tile * PACK

    low_ids = [to_low(iota(t)) for t in range(field // PACK)]
    high_ids = []
    for t in range(height // PACK):
        within = iota(t) % TILE
        high_ids.append(to_low(jnp.where(within < fine_rows, iota(t) // TILE * fine_rows + within, -1)))
    both_ids = []
    is_weight = {}
    for t in range(tall // PACK):
        peer = iota(t) // group
        both_ids.append(to_low(jnp.where(peer < peers, peer * fine_rows + iota(t) % fine_rows, -1)))
        is_weight[t * PACK % group] = to_low(jnp.where(iota(t) % group < fine_rows, 1, 0)) > 0.5
    one = jnp.ones((PACK, SPAN), jnp.bfloat16)
    zero = jnp.zeros((PACK, SPAN), jnp.bfloat16)

    def hot(ids, where, filled):
        return jnp.concatenate([jnp.where(i == where, f, zero) for i, f in zip(ids, filled)], axis=0)

    def spread(ref, row):
        return jnp.broadcast_to(ref[pl.ds(row, 1), :], (PACK, SPAN)).astype(jnp.bfloat16)

    def contract(left, right):
        return lax.dot_general(
            jnp.concatenate(left, axis=1),
            jnp.concatenate(right, axis=1),
            (((1,), (1,)), ((), ())),
            preferred_element_type=jnp.float32,
        )

    ones = [one] * len(low_ids)
    chunk = min(EARLY, detectors)

    def early_step(i, sums):
        base = pl.multiple_of(i * chunk, TILE)
        new = []
        for span in range(spans):
            left, right = [], []
            for d in range(chunk):
                right.append(hot(low_ids, spread(low_ref.at[span], base + d), ones))
                weight = spread(weight_rows, base + d)
                mixed = {k: jnp.where(mask, weight, one) for k, mask in is_weight.items()}
                filled = [mixed[t * PACK % group] for t in range(len(both_ids))]
                left.append(hot(both_ids, spread(high_ref.at[span], base + d), filled))
            new.append(sums[span] + contract(left, right))
        return tuple(new)

    start = tuple(jnp.zeros((tall, field), jnp.float32) for _ in range(spans))
    sums = lax.fori_loop(0, detectors // chunk, early_step, start)
    early_flat[...] = jnp.concatenate(sums, axis=1)

    lane = lax.broadcasted_iota(jnp.int32, (1, SPAN), 1)
    loads[3].wait()
    label = jnp.zeros((1, SPAN), jnp.float32)
    for span in range(spans):
        label = jnp.where(lane >= span * field, span_block_ref[span, det].astype(jnp.float32), label)
    for p in range(peers):
        early_out[p, :group] = early_flat[p * group : (p + 1) * group]
        early_out[p, group : group + 1] = label

    slot_of = {offset: n for n, offset in enumerate(others)}

    def send(source, landing, send_sem, recv_sem, count):
        for offset in others:
            to = target(offset)
            pltpu.make_async_remote_copy(
                src_ref=source.at[to["det"] * nsub + to["sub"], *count],
                dst_ref=landing.at[slot_of[offset], *count],
                send_sem=send_sem,
                recv_sem=recv_sem,
                device_id=to,
                device_id_type=MESH,
            ).start()

    own_place = det * nsub + sub
    remote = len(others)

    pl.semaphore_wait(passed, len(plane))
    early_used = (pl.ds(0, group + 1),)
    send(early_out, early_in, early_send, early_recv, early_used)

    total = jnp.sum(picked, axis=1, keepdims=True)
    late_chunk = min(LATE, detectors)

    def value_sums(span, i, sums):
        base = pl.multiple_of(i * late_chunk, TILE)
        new = []
        for half in range(2):
            left, right = [], []
            for n in range(late_chunk // 2):
                d = base + half * (late_chunk // 2) + n
                right.append(hot(low_ids, spread(low_ref.at[span], d), ones))
                value = spread(value_ref.at[span], d)
                left.append(hot(high_ids, spread(high_ref.at[span], d), [value] * len(high_ids)))
            new.append(sums[half] + contract(left, right))
        return tuple(new)

    def arrived(span):
        gone = tod_all.at[pl.ds(0, ndet - 1), span]
        pltpu.make_async_copy(gone, gone, tod_recv.at[span]).wait()

    for span in range(spans):
        arrived(span)
        folded = jnp.zeros((TILE, SPAN), jnp.float32)
        for q in range(ndet):
            weighted = tod_all[q, span] * weight_rows[q * mine : (q + 1) * mine]
            for k in range(mine // TILE):
                folded = folded + weighted[k * TILE : (k + 1) * TILE]
        shift = 1
        while shift < TILE:
            folded = folded + pltpu.roll(folded, shift, 0)
            shift *= 2
        repeated = jnp.concatenate([folded / total] * (mine // TILE), axis=0)
        for q in range(ndet):
            piece = slice(q * mine, (q + 1) * mine)
            clean = tod_all[q, span] - repeated
            if q * mine % late_chunk >= late_chunk // 2:
                clean = repeated - tod_all[q, span]
            value_ref[span, piece] = weight_rows[piece] * clean
        halves = lax.fori_loop(
            0,
            detectors // late_chunk,
            functools.partial(value_sums, span),
            tuple(jnp.zeros((height, field), jnp.float32) for _ in range(2)),
        )
        held[span] = halves[0] - halves[1]
    signal = jnp.concatenate([held[span] for span in range(spans)], axis=1)
    for p in range(peers):
        late_out[p] = signal[p * TILE : (p + 1) * TILE]
    used = (pl.ds(0, fine_rows),)
    send(late_out, late_in, late_send, late_recv, used)
    late_in[remote] = late_out[own_place]
    early_in[remote] = early_out[own_place]

    def finish(copy_sem, landing):
        pltpu.make_async_copy(landing, landing, copy_sem).wait()

    early_all = early_in.at[pl.ds(0, remote), *early_used]
    late_all = late_in.at[pl.ds(0, remote), *used]
    first = (blk * BLK_OWN).astype(jnp.float32)

    def gather(tiles_of):
        def step(n, acc):
            label = jnp.broadcast_to(early_in[n, pl.ds(group, 1), :], (TILE, SPAN))
            acc = list(acc)
            for b in range(BLK_OWN):
                mine_here = label == first + b
                for k, tile in enumerate(tiles_of(n)):
                    at = k * BLK_OWN + b
                    acc[at] = acc[at] + jnp.where(mine_here, tile, 0.0)
            return tuple(acc)

        kinds = len(tiles_of(0))
        acc = tuple(jnp.zeros((TILE, SPAN), jnp.float32) for _ in range(kinds * BLK_OWN))
        if total_peers <= 16:
            for n in range(total_peers):
                acc = step(n, acc)
            return acc
        return lax.fori_loop(0, total_peers, step, acc)

    def put(kind, tiles, top=0):
        for b, tile in enumerate(tiles):
            whole = tile
            for span in range(1, spans):
                whole = whole + pltpu.roll(tile, span * field, 1)
            for r in range(fine_rows):
                skip = r * fine % SPAN // field * field
                skip = skip if skip + fine <= SPAN else 0
                line = whole[top + r : top + r + 1, skip : skip + fine]
                out_ref[kind, b : b + 1, r * fine : (r + 1) * fine] = line

    finish(early_recv, early_all)
    acc = gather(lambda n: (early_in[n, :TILE], early_in[n, TILE:]))
    tiles = [jnp.concatenate([acc[b], acc[BLK_OWN + b]], axis=0) for b in range(BLK_OWN)]
    put(1, tiles)
    put(2, tiles, fine_rows)

    finish(late_recv, late_all)
    put(0, gather(lambda n: (late_in[n],)))

    tod_gone = tod_all.at[pl.ds(0, ndet - 1)]
    finish(tod_send, tod_gone)
    finish(early_send, early_all)
    finish(late_send, late_all)


def on_device(tod, pixels, span_block, weight_class, class_weight):
    ndet, nblk, nsub = (lax.axis_size(a) for a in ("det", "blk", "sub"))
    mine, segments, samples = tod.shape
    detectors = pixels.shape[0]
    spans = samples // SPAN
    peers = ndet * nsub
    slots = peers * nblk
    width = BLOCK_PIX // peers
    lanes = next(n for n in range(SPAN, 0, -1) if width % n == 0)
    rows = width // lanes
    assert segments == ndet and detectors == ndet * mine
    assert TILE % spans == 0 and 2 * rows < TILE and lanes % 2 == 0 and lanes // 2 <= SPAN // spans
    flat = (detectors * spans, SPAN)
    vmem = pl.BlockSpec(memory_space=pltpu.VMEM)
    hbm = pl.BlockSpec(memory_space=pl.ANY)
    f32 = jnp.float32
    dma = pltpu.SemaphoreType.DMA
    out = pl.pallas_call(
        functools.partial(kernel, (ndet, nblk, nsub, spans, lanes, rows)),
        out_shape=pltpu.VMEM((3, BLK_OWN, width), f32),
        in_specs=[hbm] * 5,
        out_specs=vmem,
        scratch_shapes=[
            pltpu.VMEM((1, detectors), jnp.int32),
            pltpu.SMEM(class_weight.shape, f32),
            pltpu.SMEM((spans, segments), jnp.int32),
            pltpu.VMEM(flat, jnp.int32),
            pltpu.VMEM((ndet, spans, mine, SPAN), f32),
            pltpu.VMEM((ndet, spans, mine, SPAN), f32),
            pltpu.VMEM((spans, detectors, SPAN), f32),
            pltpu.VMEM((spans, detectors, SPAN), f32),
            pltpu.VMEM((detectors, SPAN), f32),
            pltpu.VMEM((spans, detectors, SPAN), f32),
            pltpu.VMEM((-(-peers * 4 * rows // PACK) * PACK, SPAN), f32),
            pltpu.VMEM((spans, peers * TILE, SPAN // spans), f32),
            pltpu.VMEM((peers, PACK, SPAN), f32),
            pltpu.VMEM((slots, PACK, SPAN), f32),
            pltpu.VMEM((peers, TILE, SPAN), f32),
            pltpu.VMEM((slots, TILE, SPAN), f32),
            dma((5,)),
            dma,
            dma((spans,)),
            dma,
            dma,
            dma,
            dma,
            pltpu.SemaphoreType.REGULAR,
        ],
        compiler_params=pltpu.CompilerParams(collective_id=0, has_side_effects=True),
    )(
        tod,
        pixels.reshape(flat),
        weight_class.reshape(1, detectors),
        class_weight,
        span_block.T,
    )
    return (out[0], out[1], out[2])


def solution(mesh):
    placed = (
        P(("groups", "det"), None, ("blk", "sub")),
        P("groups", "det", ("blk", "sub")),
        P("groups", ("blk", "sub")),
        P("groups"),
        P("groups"),
    )
    sliced = P(("groups", "blk"), ("det", "sub"))
    return jax.shard_map(
        on_device,
        mesh=mesh,
        in_specs=placed,
        out_specs=(sliced, sliced, sliced),
        check_vma=False,
    )
```
